32 devices in a mesh: section: 4 (over y, x), mp: 8 (over z, core).
Axes of the slice: x: 2, y: 2, z: 4, core: 2. Of those that a mesh axis runs over, the one named last changes fastest.
Arguments:
- stream: bfloat16 [512, 4096], P(('section', 'mp')), may hold values from -6 to 6
- ffn_gain: float32 [4096], replicated, may hold values from 0.25 to 1.75
- router_weight: bfloat16 [4096, 4], replicated, may hold values from -0.1875 to 0.1875
- expert_ids: int32 [512, 2], P(('section', 'mp')), may hold values from 0 to 3, all different within a row; in each aligned block of 16 rows (0 to 15, 16 to 31, ...) at most 12 rows name the same one
- w_gate: bfloat16 [4, 4096, 14336], P('section', None, 'mp'), may hold values from -0.09375 to 0.09375
- w_up: bfloat16 [4, 4096, 14336], P('section', None, 'mp'), may hold values from -0.09375 to 0.09375
- w_down: bfloat16 [4, 14336, 4096], P('section', 'mp'), may hold values from -0.09375 to 0.09375
- attn_gain: float32 [4096], replicated, may hold values from 0.25 to 1.75
- w_kv: bfloat16 [4096, 2048], P(None, 'mp'), may hold values from -0.09375 to 0.09375
Outputs:
- stream_out: bfloat16 [512, 4096], P(('section', 'mp'))
- kv_decode: bfloat16 [512, 2048], P('section', 'mp')
The draws below stay inside these ranges and needn't reach their ends.
Inputs may be any that keep to these rules, and one draw needn't show every extreme that they name: `expert_ids`: each row names two different experts. Among the rows of one device no expert is named more than 12 times, a bound that some block reaches.
All inputs are finite; a program needn't handle non-finite values.
Results may differ from the reference program's by a relative error of at most 0.02.
Values may be sent and summed in bfloat16 or wider, within the bound.
A program may use at most 128 MiB of HBM per device.

```python
import math
import jax
import jax.numpy as jnp
import numpy as np
from jax import lax

D = 4096
FF = 14336
TOK_DEV = 16
EXPERTS = 4
CAP = 12
KVW = 2048
TOKENS = 512
N_MP = 8


def steps_of(key, shape, split, least, largest):
    factor_of = 1.0
    for axis_at, shards_of in split:
        draws = jax.random.uniform(jax.random.fold_in(jax.random.fold_in(key, 6), axis_at), (shards_of,), jnp.float32, least / len(split), largest / len(split))
        factor_of = factor_of * jnp.repeat(jnp.exp(draws), shape[axis_at] // shards_of).reshape((-1,) + (1,) * (len(shape) - 1 - axis_at))
    return factor_of


def deal_out(rng, own, number, rows, count, top, reach, skew):
    sequence = jax.random.permutation(rng, count)
    crowded, common = portions_of(count, rows * top, reach, skew, True), portions_of(count, rows * top, reach, skew, False)
    places = jnp.arange(count)

    def named(sizes, turn):
        used = int((sizes > 0).sum())
        fixed = max(1, used // 4)
        moved = fixed + (places - fixed + turn * (used - fixed)) % max(1, count - fixed)
        return jnp.zeros((count,), jnp.int32).at[sequence[jnp.where(places < fixed, places, moved)]].set(jnp.asarray(sizes, jnp.int32))

    sizes = jnp.where(number % 4 == 0, named(crowded, number // 4), named(common, number - number // 4 - 1))
    mixed = jax.random.permutation(jax.random.fold_in(own, 3), count)
    source_of, taker = mixed[0:count // 2 * 2:2], mixed[1:count // 2 * 2:2]
    margin = jnp.minimum(sizes[source_of] - 1, reach - sizes[taker]) // 2
    margin = jnp.where((source_of == sequence[0]) | (taker == sequence[0]) | (sizes[taker] == 0), 0, jnp.maximum(margin, 0))
    moved = jax.random.randint(jax.random.fold_in(own, 4), (count // 2,), 0, 1 << 20) % (margin + 1)
    sizes = sizes.at[source_of].add(-moved).at[taker].add(moved)
    items = jnp.searchsorted(jnp.cumsum(sizes), jnp.arange(rows * top), side="right").astype(jnp.int32)
    listing = items.reshape(top, rows).T
    listing = listing[jax.random.permutation(jax.random.fold_in(own, 1), rows)]
    turn = jax.random.randint(jax.random.fold_in(own, 2), (rows, 1), 0, top)
    return jnp.take_along_axis(listing, (jnp.arange(top)[None, :] + turn) % top, axis=1)


def portions_of(number_of, total, bound, lean, full):
    loads = [(1 << 20) // math.isqrt(rank ** lean) + 1 for rank in range(1, number_of + 1)]
    largest = bound if full else min(bound, max(-(-total // number_of), total * loads[0] // sum(loads)))
    least = 1 if total - largest >= number_of - 1 else 0
    holding, spare = [largest] + [least] * (number_of - 1), total - largest - least * (number_of - 1)
    while spare > 0:
        free = [i for i in range(1, number_of) if holding[i] < largest] or [i for i in range(1, number_of) if holding[i] < bound]
        mass, left = sum([loads[i] for i in free]), spare
        for i in free:
            extra = min(bound - holding[i], max(1, left * loads[i] // mass), spare)
            holding[i] = holding[i] + extra
            spare = spare - extra
    return np.array(holding)


def normal_values(key, extent, scale, limit, cuts=(), kind=jnp.bfloat16):
    entries = jax.random.normal(key, extent, jnp.float32) * scale
    if len(cuts) > 0:
        entries = steps_of(key, extent, cuts, -0.22, 0.18) * entries
    return jnp.clip(entries, min=-limit, max=limit).astype(kind)


def setup_inputs(seed: int = 0) -> dict:
    keys = jax.random.split(jax.random.key(seed), 10)
    stream = normal_values(keys[0], (TOKENS, D), 1.0, 6.0, ((0, 32),))
    ffn_gain = jnp.clip(1.0 + 0.15 * jax.random.normal(keys[1], (D,), jnp.float32), 0.25, 1.75)
    router_weight = normal_values(keys[2], (D, EXPERTS), (D // 4) ** -0.5, 0.1875)
    expert_ids_keys = jax.random.split(jax.random.fold_in(keys[3], 1), TOKENS // TOK_DEV)
    expert_ids_turns = jax.random.permutation(jax.random.fold_in(keys[3], 3), TOKENS // TOK_DEV)
    expert_ids = jax.vmap(lambda own, number: deal_out(jax.random.fold_in(keys[3], 2), own, number, TOK_DEV, EXPERTS, 2, CAP, 2))(expert_ids_keys, expert_ids_turns).reshape((TOKENS, 2))
    w_gate = normal_values(keys[4], (EXPERTS, D, FF), D ** -0.5, 0.09375, ((0, 4), (2, 8)))
    w_up = normal_values(keys[5], (EXPERTS, D, FF), D ** -0.5, 0.09375, ((0, 4), (2, 8)))
    w_down = normal_values(keys[6], (EXPERTS, FF, D), (FF // 4) ** -0.5, 0.09375, ((0, 4), (1, 8)))
    attn_gain = jnp.clip(1.0 + 0.15 * jax.random.normal(keys[7], (D,), jnp.float32), 0.25, 1.75)
    w_kv = normal_values(keys[8], (D, KVW), D ** -0.5, 0.09375, ((1, 8),))
    return dict(stream=stream, ffn_gain=ffn_gain, router_weight=router_weight, expert_ids=expert_ids, w_gate=w_gate, w_up=w_up, w_down=w_down, attn_gain=attn_gain, w_kv=w_kv)


epsilon = 1e-05

def normalize(values, scale_gain):
    floats = values.astype(jnp.float32)
    return floats * lax.rsqrt(lax.optimization_barrier(jnp.mean(floats * floats, axis=-1, keepdims=True)) + epsilon) * scale_gain

def reference(stream, ffn_gain, router_weight, expert_ids, w_gate, w_up, w_down, attn_gain, w_kv):
    tokens = stream.shape[0]
    blocks = tokens // TOK_DEV
    normed = normalize(stream, ffn_gain).astype(jnp.bfloat16)
    logits = jnp.dot(normed, router_weight, preferred_element_type=jnp.float32)
    onehot = expert_ids[:, :, None] == jnp.arange(EXPERTS, dtype=jnp.int32)[None, None, :]
    chosen = lax.optimization_barrier(jnp.sum(jnp.where(onehot, logits[:, None, :], jnp.float32(0.0)), axis=-1))
    share_first = jax.nn.sigmoid(chosen[:, 0] - chosen[:, 1])
    flat_hits = onehot.reshape(blocks, TOK_DEV * 2, EXPERTS).astype(jnp.int32)
    before = jnp.cumsum(flat_hits, axis=1) - flat_hits
    slot_index = lax.optimization_barrier(jnp.sum(before * flat_hits, axis=-1)).reshape(tokens, 2)
    position = (jnp.arange(tokens, dtype=jnp.int32) // TOK_DEV)[:, None] * CAP + slot_index
    repeated = jnp.repeat(normed, 2, axis=0)
    block_width = FF // N_MP
    total = jnp.zeros((tokens, 2, D), jnp.float32)
    for expert in range(EXPERTS):
        target_index = jnp.where(expert_ids == expert, position, blocks * CAP).astype(jnp.int32)
        buffer = jnp.zeros((blocks * CAP, D), jnp.bfloat16).at[target_index.reshape(-1)].set(repeated, mode='drop')
        gate_part = jnp.dot(buffer, w_gate[expert], preferred_element_type=jnp.float32)
        up_part = jnp.dot(buffer, w_up[expert], preferred_element_type=jnp.float32)
        hidden = (jax.nn.silu(gate_part) * up_part).astype(jnp.bfloat16)
        hidden_blocks = hidden.reshape(blocks * CAP, N_MP, block_width).transpose(1, 0, 2)
        down_blocks = w_down[expert].reshape(N_MP, block_width, D)

        def add_block(carry, pair):
            product = jnp.dot(pair[0], pair[1], preferred_element_type=jnp.float32)
            rounded = lax.optimization_barrier(product.astype(jnp.bfloat16))
            return (carry + rounded.astype(jnp.float32), None)
        summed, unused = lax.scan(add_block, jnp.zeros((blocks * CAP, D), jnp.float32), (hidden_blocks, down_blocks))
        result_rows = summed.astype(jnp.bfloat16)
        safe_index = jnp.clip(target_index, 0, blocks * CAP - 1)
        picked = result_rows[safe_index.reshape(-1)].reshape(tokens, 2, D).astype(jnp.float32)
        total = total + jnp.where((expert_ids == expert)[:, :, None], picked, jnp.float32(0.0))
    updated = stream.astype(jnp.float32) + share_first[:, None] * total[:, 0] + (1.0 - share_first)[:, None] * total[:, 1]
    stream_out = updated.astype(jnp.bfloat16)
    attn_input = normalize(stream_out, attn_gain).astype(jnp.bfloat16)
    kv_local = jnp.dot(attn_input, w_kv, preferred_element_type=jnp.float32).astype(jnp.bfloat16)
    kv_decode = jnp.roll(kv_local, TOK_DEV * N_MP, axis=0)
    return (stream_out, kv_decode)
```

```python
import functools

import jax
import jax.numpy as jnp
from jax import lax
from jax.experimental import pallas as pl
from jax.experimental.pallas import tpu as pltpu
from jax.sharding import PartitionSpec as P

epsilon = 1e-05


def shifted(value, axis, steps):
    count = lax.axis_size(axis)
    pairs = [(source, (source + steps) % count) for source in range(count)]
    return lax.ppermute(value, axis, pairs)


def normalize(values, scale_gain):
    floats = values.astype(jnp.float32)
    return (
        floats * lax.rsqrt(jnp.mean(floats * floats, axis=-1, keepdims=True) + epsilon) * scale_gain
    )


def plain_body(stream, ffn_gain, router_weight, expert_ids, w_gate, w_up, w_down, attn_gain, w_kv):
    own_rows = stream.shape[0]
    model_width = stream.shape[1]
    experts = router_weight.shape[1]
    capacity = min(own_rows, 3 * own_rows // experts)
    normed = normalize(stream, ffn_gain).astype(jnp.bfloat16)
    logits = jnp.dot(normed, router_weight, preferred_element_type=jnp.float32)
    onehot = expert_ids[:, :, None] == jnp.arange(experts, dtype=jnp.int32)[None, None, :]
    chosen = jnp.sum(jnp.where(onehot, logits[:, None, :], jnp.float32(0.0)), axis=-1)
    share_first = jax.nn.sigmoid(chosen[:, 0] - chosen[:, 1])
    flat_hits = onehot.reshape(own_rows * 2, experts).astype(jnp.int32)
    before = jnp.cumsum(flat_hits, axis=0) - flat_hits
    slot_index = jnp.sum(before * flat_hits, axis=-1)
    expert_flat = expert_ids.reshape(-1)
    route_table = (
        expert_flat[None, None, :] == jnp.arange(experts, dtype=jnp.int32)[:, None, None]
    ) & (slot_index[None, None, :] == jnp.arange(capacity, dtype=jnp.int32)[None, :, None])
    route_table = route_table.astype(jnp.bfloat16)
    repeated = jnp.repeat(normed, 2, axis=0)
    buffer = jnp.einsum(
        "ecr,rd->ecd", route_table, repeated, preferred_element_type=jnp.float32
    ).astype(jnp.bfloat16)
    arrived = lax.all_to_all(buffer, "section", split_axis=0, concat_axis=0, tiled=True)
    inbound = arrived.reshape(experts * capacity, model_width)
    gate_weight = w_gate[0]
    up_weight = w_up[0]
    down_weight = w_down[0]
    block_rows = lax.all_gather(inbound, "mp", axis=0, tiled=True)
    gate_part = jnp.dot(block_rows, gate_weight, preferred_element_type=jnp.float32)
    up_part = jnp.dot(block_rows, up_weight, preferred_element_type=jnp.float32)
    hidden_all = (jax.nn.silu(gate_part) * up_part).astype(jnp.bfloat16)
    block_rows = hidden_all
    summed = lax.psum_scatter(
        jnp.dot(block_rows, down_weight, preferred_element_type=jnp.float32).astype(jnp.bfloat16),
        "mp",
        scatter_dimension=0,
        tiled=True,
    )
    results = summed.reshape(experts, capacity, model_width)
    returned = lax.all_to_all(results, "section", split_axis=0, concat_axis=0, tiled=True)
    picked = jnp.einsum("ecr,ecd->rd", route_table, returned, preferred_element_type=jnp.float32)
    picked = picked.reshape(own_rows, 2, model_width)
    updated = (
        stream.astype(jnp.float32)
        + share_first[:, None] * picked[:, 0]
        + (1.0 - share_first)[:, None] * picked[:, 1]
    )
    stream_out = updated.astype(jnp.bfloat16)
    attn_input = normalize(stream_out, attn_gain).astype(jnp.bfloat16)
    kv_local = jnp.dot(
        lax.all_gather(attn_input, "mp", axis=0, tiled=True),
        w_kv,
        preferred_element_type=jnp.float32,
    ).astype(jnp.bfloat16)
    kv_decode = shifted(kv_local, "section", 1)
    return (stream_out, kv_decode)


MESH = pl.DeviceIdType.MESH
f32, bf16 = jnp.float32, jnp.bfloat16
SLOTS = 4
VMEM_BYTES = 67043328
LANES = 128


def fused_kernel(
    sections, layers, chunks,
    stream, ffn_gain, router_t, ids, attn_gain, wg_hbm, wu_hbm, wd_hbm, wkv_hbm,
    out, kv_out,
    x_all, mix_all, wg, wu, wd, wkv, gate, up, hidden, part, pair_in, xd_in, yd_in, x_in, y_in, z_in,
    attn, kv_mine, kv_in, weight,
    g_send, g_recv, r_send, r_recv, w_sem, d_sem, k_send, k_recv,
):
    own, width = stream.shape
    cc = width // chunks
    rows = 2 * sections * layers * own
    hid = hidden.shape[1]
    tile = 256 if hid % 256 == 0 else LANES
    s, m = lax.axis_index("section"), lax.axis_index("mp")
    z, k = m // 2, m % 2
    x, y = s % 2, s // 2
    sx, sy, sd = y * 2 + (1 - x), (1 - y) * 2 + x, (1 - y) * 2 + (1 - x)
    half = layers // 2
    to_x, to_y = {"section": sx, "mp": m}, {"section": sy, "mp": m}
    partner = {"section": s, "mp": z * 2 + 1 - k}

    def z_peer(d):
        return (z + d) % layers

    def z_dev(d):
        return {"section": s, "mp": z_peer(d) * 2 + k}

    def load(c):
        slot = c % SLOTS
        at = pl.ds(c * cc, cc)
        return (
            pltpu.make_async_copy(wg_hbm.at[0, at], wg.at[slot], w_sem.at[slot, 0]),
            pltpu.make_async_copy(wu_hbm.at[0, at], wu.at[slot], w_sem.at[slot, 1]),
        )

    def load_down():
        return (
            pltpu.make_async_copy(wd_hbm.at[0], wd, d_sem.at[0]),
            pltpu.make_async_copy(wkv_hbm, wkv, d_sem.at[1]),
        )

    for c in range(min(SLOTS, chunks)):
        for copy in load(c):
            copy.start()

    barrier = pltpu.get_barrier_semaphore()
    greet = [z_dev(d) for d in range(1, layers)] + [partner]
    greet += [{"section": (s + d) % sections, "mp": m} for d in range(1, sections)]
    for dev in greet:
        pl.semaphore_signal(barrier, inc=1, device_id=dev, device_id_type=MESH)

    floats = stream[...].astype(f32)
    normed = floats * lax.rsqrt(jnp.mean(floats * floats, axis=-1, keepdims=True) + epsilon)
    normed = (normed * ffn_gain[...]).astype(bf16)
    for c in range(chunks):
        x_all[c, k, s, z] = normed[:, c * cc : (c + 1) * cc]
    wide = normed.astype(f32)
    lane = lax.broadcasted_iota(jnp.int32, (own, LANES), 1)
    first, second = ids[:, 0:1], ids[:, 1:2]
    la, lb = jnp.zeros((own, 1), f32), jnp.zeros((own, 1), f32)
    for e in range(router_t.shape[0]):
        logit = jnp.sum(wide * router_t[e : e + 1, :].astype(f32), axis=-1, keepdims=True)
        la = la + jnp.where(first == e, logit, 0.0)
        lb = lb + jnp.where(second == e, logit, 0.0)
    share = jax.nn.sigmoid(la - lb)
    mix = jnp.where(lane == first, share, 0.0) + jnp.where(lane == second, 1.0 - share, 0.0)
    high = mix.astype(bf16)
    mix_all[k, s, z, :, 0:LANES] = high
    mix_all[k, s, z, :, LANES : 2 * LANES] = (mix - high.astype(f32)).astype(bf16)
    pl.semaphore_wait(barrier, len(greet))

    pieces = [x_all.at[0], mix_all] + [x_all.at[c] for c in range(1, chunks)]
    chunk_of = [0, None] + list(range(1, chunks))
    count = len(pieces)
    sent = []

    def remote(src, dst, ss, rs, dev):
        return pltpu.make_async_remote_copy(
            src_ref=src, dst_ref=dst, send_sem=ss, recv_sem=rs, device_id=dev, device_id_type=MESH
        )

    def go(copy):
        copy.start()
        sent.append(copy)

    def gz(i, d):
        ref = pieces[i].at[k, s, z]
        return remote(ref, ref, g_send.at[i, d - 1], g_recv.at[i, d - 1], z_dev(d))

    base = layers - 1

    def gcopy(i, j, ref, dev):
        return remote(ref, ref, g_send.at[i, base + j], g_recv.at[i, base + j], dev)

    def gx(i):
        return gcopy(i, 0, pieces[i].at[k, s], to_x)

    def gy(i):
        return gcopy(i, 1, pieces[i].at[k, s], to_y)

    def gfy(i):
        return gcopy(i, 2, pieces[i].at[k, sx, pl.ds(0, half)], to_y)

    def gfx(i):
        return gcopy(i, 3, pieces[i].at[k, sy, pl.ds(half, layers - half)], to_x)

    def gp(i, j):
        return gcopy(i, 4 + j, pieces[i].at[k, (s, sx, sy, sd)[j]], partner)

    for i in range(count):
        for d in range(1, layers):
            go(gz(i, d))

    def gather_steps(t):
        if t < count:
            for d in range(1, layers):
                gz(t, d).wait_recv()
            go(gx(t))
            go(gy(t))
            go(gp(t, 0))
        if 0 <= t - 1 < count:
            gx(t - 1).wait_recv()
            go(gfy(t - 1))
            go(gp(t - 1, 1))
            gy(t - 1).wait_recv()
            go(gfx(t - 1))
            go(gp(t - 1, 2))
        if 0 <= t - 2 < count:
            gfy(t - 2).wait_recv()
            gfx(t - 2).wait_recv()
            go(gp(t - 2, 3))
        if 0 <= t - 3 < count:
            for j in range(4):
                gp(t - 3, j).wait_recv()

    def gate_up(c):
        slot = c % SLOTS
        for copy in load(c):
            copy.wait()

        def step(n, carry):
            at = pl.ds(pl.multiple_of(n * tile, tile), tile)
            tokens = x_all[c].reshape(rows, cc)
            g = jnp.dot(tokens, wg[slot, :, at], preferred_element_type=f32)
            u = jnp.dot(tokens, wu[slot, :, at], preferred_element_type=f32)
            if c > 0:
                g = g + gate[:, at]
                u = u + up[:, at]
            if c < chunks - 1:
                gate[:, at] = g
                up[:, at] = u
            else:
                hidden[:, at] = (g / (1.0 + jnp.exp(-g)) * u * weight[:, 0:1]).astype(bf16)
            return carry

        lax.fori_loop(0, hid // tile, step, 0)
        if c + SLOTS < chunks:
            for copy in load(c + SLOTS):
                copy.start()

    for t in range(count + 3):
        gather_steps(t)
        if t == 3:
            for copy in load_down():
                copy.start()
        if t >= 3:
            c = chunk_of[t - 3]
            if c is None:
                both = mix_all[...].reshape(rows, 2 * LANES).astype(f32)
                both = both[:, 0:LANES] + both[:, LANES : 2 * LANES]
                at_lane = lax.broadcasted_iota(jnp.int32, (rows, LANES), 1)
                mine = jnp.sum(jnp.where(at_lane == s, both, 0.0), axis=-1, keepdims=True)
                weight[...] = jnp.broadcast_to(mine, (rows, LANES))
            else:
                gate_up(c)

    def rcopy(c, j, src, dst, dev):
        return remote(src, dst, r_send.at[c, j], r_recv.at[c, j], dev)

    def r_pair(c):
        return rcopy(c, 0, part.at[c, 1 - k], pair_in.at[c], partner)

    def r_xd(c):
        return rcopy(c, 1, part.at[c, k, sd, pl.ds(0, half)], xd_in.at[c], to_x)

    def r_yd(c):
        return rcopy(c, 2, part.at[c, k, sd, pl.ds(half, layers - half)], yd_in.at[c], to_y)

    def r_x(c):
        return rcopy(c, 3, part.at[c, k, sx], x_in.at[c], to_x)

    def r_y(c):
        return rcopy(c, 4, part.at[c, k, sy], y_in.at[c], to_y)

    def r_z(c, d):
        return rcopy(c, 5 + d, part.at[c, k, s, z_peer(d)], z_in.at[c, d - 1], z_dev(d))

    def a_z(c, d):
        ref = attn.at[c, k, z]
        return rcopy(c, 5 + base + d, ref, ref, z_dev(d))

    def a_pair(c):
        ref = attn.at[c, k]
        return rcopy(c, 5, ref, ref, partner)

    def down(c):
        for n in range(cc // tile):
            lo = c * cc + n * tile
            r = jnp.dot(hidden[...], wd[:, lo : lo + tile], preferred_element_type=f32)
            part[c, :, :, :, :, n * tile : (n + 1) * tile] = r.astype(bf16).reshape(
                2, sections, layers, own, tile
            )

    def plus(a, b):
        return (a.astype(f32) + b.astype(f32)).astype(bf16)

    group = 2 * layers * own
    state = {"kv": jnp.zeros((group, wkv.shape[1]), f32), "ss": jnp.zeros((group, 1), f32)}

    for copy in load_down():
        copy.wait()
    for t in range(chunks + 6):
        if 0 <= t - 5 < chunks:
            for d in range(1, layers):
                a_z(t - 5, d).wait_recv()
            go(a_pair(t - 5))
        if 0 <= t - 4 < chunks:
            c = t - 4
            cols = slice(c * cc, (c + 1) * cc)
            total = part[c, k, s, z].astype(f32)
            for d in range(1, layers):
                r_z(c, d).wait_recv()
                total = total + z_in[c, d - 1].astype(f32)
            updated = (stream[:, cols].astype(f32) + total).astype(bf16)
            attn[c, k, z] = updated
            for d in range(1, layers):
                go(a_z(c, d))
            out[:, cols] = updated
        if 0 <= t - 3 < chunks:
            c = t - 3
            r_x(c).wait_recv()
            r_y(c).wait_recv()
            add = part[c, k, s].astype(f32) + x_in[c].astype(f32) + y_in[c].astype(f32)
            part[c, k, s] = add.astype(bf16)
            for d in range(1, layers):
                go(r_z(c, d))
        if 0 <= t - 2 < chunks:
            c = t - 2
            r_xd(c).wait_recv()
            part[c, k, sy, 0:half] = plus(part[c, k, sy, 0:half], xd_in[c])
            go(r_y(c))
            r_yd(c).wait_recv()
            part[c, k, sx, half:layers] = plus(part[c, k, sx, half:layers], yd_in[c])
            go(r_x(c))
        if 0 <= t - 1 < chunks:
            c = t - 1
            r_pair(c).wait_recv()
            part[c, k] = plus(part[c, k], pair_in[c])
            go(r_xd(c))
            go(r_yd(c))
        if t < chunks:
            down(t)
            go(r_pair(t))
        if 0 <= t - 5 < chunks:
            c = t - 5
            cols = slice(c * cc, (c + 1) * cc)
            a_pair(c).wait_recv()
            values = attn[c].reshape(group, cc).astype(f32)
            state["ss"] = state["ss"] + jnp.sum(values * values, axis=-1, keepdims=True)
            scaled = (values * attn_gain[:, cols]).astype(bf16)
            state["kv"] = state["kv"] + jnp.dot(scaled, wkv[cols, :], preferred_element_type=f32)
    keys = state["kv"] * lax.rsqrt(state["ss"] / width + epsilon)
    keys = keys.astype(bf16).reshape(2, layers, own, wkv.shape[1])
    for core in range(2):
        for layer in range(layers):
            at = (layer * 2 + core) * own
            kv_mine[at : at + own, :] = keys[core, layer]
    onward = remote(
        kv_mine, kv_in, k_send.at[0], k_recv.at[0], {"section": (s + 1) % sections, "mp": m}
    )
    go(onward)
    onward.wait_recv()
    kv_out[...] = kv_in[...]
    for copy in sent:
        copy.wait_send()


def fused_body(sections, mp, chunks, stream, ffn_gain, router_weight, expert_ids, w_gate, w_up, w_down, attn_gain, w_kv):
    own, width = stream.shape
    layers = mp // 2
    cc = width // chunks
    hid = w_gate.shape[2]
    rows = sections * mp * own
    kvc = w_kv.shape[1]
    vmem = pl.BlockSpec(memory_space=pltpu.VMEM)
    hbm = pl.BlockSpec(memory_space=pl.ANY)
    dma = pltpu.SemaphoreType.DMA
    gathers, returns = layers - 1 + 8, 5 + 2 * layers - 1
    flops = 6 * rows * width * hid
    return pl.pallas_call(
        functools.partial(fused_kernel, sections, layers, chunks),
        out_shape=(
            jax.ShapeDtypeStruct((own, width), bf16),
            jax.ShapeDtypeStruct((mp * own, kvc), bf16),
        ),
        in_specs=[vmem] * 5 + [hbm] * 4,
        out_specs=(vmem, vmem),
        scratch_shapes=[
            pltpu.VMEM((chunks, 2, sections, layers, own, cc), bf16),
            pltpu.VMEM((2, sections, layers, own, 2 * LANES), bf16),
            pltpu.VMEM((SLOTS, cc, hid), bf16),
            pltpu.VMEM((SLOTS, cc, hid), bf16),
            pltpu.VMEM((hid, width), bf16),
            pltpu.VMEM((width, kvc), bf16),
            pltpu.VMEM((rows, hid), f32),
            pltpu.VMEM((rows, hid), f32),
            pltpu.VMEM((rows, hid), bf16),
            pltpu.VMEM((chunks, 2, sections, layers, own, cc), bf16),
            pltpu.VMEM((chunks, sections, layers, own, cc), bf16),
            pltpu.VMEM((chunks, layers // 2, own, cc), bf16),
            pltpu.VMEM((chunks, layers - layers // 2, own, cc), bf16),
            pltpu.VMEM((chunks, layers, own, cc), bf16),
            pltpu.VMEM((chunks, layers, own, cc), bf16),
            pltpu.VMEM((chunks, layers - 1, own, cc), bf16),
            pltpu.VMEM((chunks, 2, layers, own, cc), bf16),
            pltpu.VMEM((mp * own, kvc), bf16),
            pltpu.VMEM((mp * own, kvc), bf16),
            pltpu.VMEM((rows, LANES), f32),
            dma((chunks + 1, gathers)),
            dma((chunks + 1, gathers)),
            dma((chunks, returns)),
            dma((chunks, returns)),
            dma((SLOTS, 2)),
            dma((2,)),
            dma((1,)),
            dma((1,)),
        ],
        compiler_params=pltpu.CompilerParams(
            collective_id=0, has_side_effects=True, vmem_limit_bytes=VMEM_BYTES
        ),
        cost_estimate=pl.CostEstimate(
            flops=flops, bytes_accessed=6 * width * hid, transcendentals=rows * hid
        ),
        name="expert_feed_forward",
    )(
        stream, ffn_gain[None, :], router_weight.T, expert_ids, attn_gain[None, :],
        w_gate, w_up, w_down, w_kv,
    )


def body(sections, mp, *args):
    stream, router_weight, w_gate = args[0], args[2], args[4]
    own, width = stream.shape
    rows, hid = sections * mp * own, w_gate.shape[2]
    chunks = width // 512
    held = rows * width * 7 + rows * hid * 10 + width * hid * 2 + SLOTS * 2048 * hid
    fits = held < VMEM_BYTES - (6 << 20)
    shaped = sections == 4 and mp % 4 == 0 and own % 16 == 0 and width % 512 == 0
    shaped = shaped and hid % LANES == 0 and router_weight.shape[1] == sections
    if fits and shaped:
        return fused_body(sections, mp, chunks, *args)
    return plain_body(*args)


def solution(mesh):
    in_specs = (
        P(("section", "mp"), None),
        P(),
        P(),
        P(("section", "mp"), None),
        P("section", None, "mp"),
        P("section", None, "mp"),
        P("section", "mp", None),
        P(),
        P(None, "mp"),
    )
    out_specs = (P(("section", "mp"), None), P("section", "mp"))
    return jax.shard_map(
        functools.partial(body, mesh.shape["section"], mesh.shape["mp"]), mesh=mesh, in_specs=in_specs, out_specs=out_specs, check_vma=False)
```

```python
import functools

import jax
import jax.numpy as jnp
from jax import lax
from jax.experimental import pallas as pl
from jax.experimental.pallas import tpu as pltpu
from jax.sharding import PartitionSpec as P

epsilon = 1e-05


def shifted(value, axis, steps):
    count = lax.axis_size(axis)
    pairs = [(source, (source + steps) % count) for source in range(count)]
    return lax.ppermute(value, axis, pairs)


def normalize(values, scale_gain):
    floats = values.astype(jnp.float32)
    return (
        floats * lax.rsqrt(jnp.mean(floats * floats, axis=-1, keepdims=True) + epsilon) * scale_gain
    )


def plain_body(stream, ffn_gain, router_weight, expert_ids, w_gate, w_up, w_down, attn_gain, w_kv):
    own_rows = stream.shape[0]
    model_width = stream.shape[1]
    experts = router_weight.shape[1]
    capacity = min(own_rows, 3 * own_rows // experts)
    normed = normalize(stream, ffn_gain).astype(jnp.bfloat16)
    logits = jnp.dot(normed, router_weight, preferred_element_type=jnp.float32)
    onehot = expert_ids[:, :, None] == jnp.arange(experts, dtype=jnp.int32)[None, None, :]
    chosen = jnp.sum(jnp.where(onehot, logits[:, None, :], jnp.float32(0.0)), axis=-1)
    share_first = jax.nn.sigmoid(chosen[:, 0] - chosen[:, 1])
    flat_hits = onehot.reshape(own_rows * 2, experts).astype(jnp.int32)
    before = jnp.cumsum(flat_hits, axis=0) - flat_hits
    slot_index = jnp.sum(before * flat_hits, axis=-1)
    expert_flat = expert_ids.reshape(-1)
    route_table = (
        expert_flat[None, None, :] == jnp.arange(experts, dtype=jnp.int32)[:, None, None]
    ) & (slot_index[None, None, :] == jnp.arange(capacity, dtype=jnp.int32)[None, :, None])
    route_table = route_table.astype(jnp.bfloat16)
    repeated = jnp.repeat(normed, 2, axis=0)
    buffer = jnp.einsum(
        "ecr,rd->ecd", route_table, repeated, preferred_element_type=jnp.float32
    ).astype(jnp.bfloat16)
    arrived = lax.all_to_all(buffer, "section", split_axis=0, concat_axis=0, tiled=True)
    inbound = arrived.reshape(experts * capacity, model_width)
    gate_weight = w_gate[0]
    up_weight = w_up[0]
    down_weight = w_down[0]
    block_rows = lax.all_gather(inbound, "mp", axis=0, tiled=True)
    gate_part = jnp.dot(block_rows, gate_weight, preferred_element_type=jnp.float32)
    up_part = jnp.dot(block_rows, up_weight, preferred_element_type=jnp.float32)
    hidden_all = (jax.nn.silu(gate_part) * up_part).astype(jnp.bfloat16)
    block_rows = hidden_all
    summed = lax.psum_scatter(
        jnp.dot(block_rows, down_weight, preferred_element_type=jnp.float32).astype(jnp.bfloat16),
        "mp",
        scatter_dimension=0,
        tiled=True,
    )
    results = summed.reshape(experts, capacity, model_width)
    returned = lax.all_to_all(results, "section", split_axis=0, concat_axis=0, tiled=True)
    picked = jnp.einsum("ecr,ecd->rd", route_table, returned, preferred_element_type=jnp.float32)
    picked = picked.reshape(own_rows, 2, model_width)
    updated = (
        stream.astype(jnp.float32)
        + share_first[:, None] * picked[:, 0]
        + (1.0 - share_first)[:, None] * picked[:, 1]
    )
    stream_out = updated.astype(jnp.bfloat16)
    attn_input = normalize(stream_out, attn_gain).astype(jnp.bfloat16)
    kv_local = jnp.dot(
        lax.all_gather(attn_input, "mp", axis=0, tiled=True),
        w_kv,
        preferred_element_type=jnp.float32,
    ).astype(jnp.bfloat16)
    kv_decode = shifted(kv_local, "section", 1)
    return (stream_out, kv_decode)


MESH = pl.DeviceIdType.MESH
f32, bf16 = jnp.float32, jnp.bfloat16
SLOTS = 4
Z_AHEAD = 3
GATHER_LAG = (2, 4, 5)
RETURN_LAG = (1, 3, 5, 7, 9, 10)
VMEM_BYTES = 67043328
LANES = 128


def fused_kernel(
    sections, layers, chunks,
    stream, ffn_gain, router_t, ids, attn_gain, wg_hbm, wu_hbm, wd_hbm, wkv_hbm,
    out, kv_out,
    x_all, mix_all, wg, wu, wd, wkv, gate, up, hidden, part, pair_in, xd_in, yd_in, x_in, y_in, z_in,
    attn, kv_mine, kv_in, weight,
    g_send, g_recv, r_send, r_recv, w_sem, d_sem, k_send, k_recv,
):
    own, width = stream.shape
    cc = width // chunks
    rows = 2 * sections * layers * own
    hid = hidden.shape[1]
    tile = 256 if hid % 256 == 0 else LANES
    s, m = lax.axis_index("section"), lax.axis_index("mp")
    z, k = m // 2, m % 2
    x, y = s % 2, s // 2
    sx, sy, sd = y * 2 + (1 - x), (1 - y) * 2 + x, (1 - y) * 2 + (1 - x)
    half = layers // 2
    to_x, to_y = {"section": sx, "mp": m}, {"section": sy, "mp": m}
    partner = {"section": s, "mp": z * 2 + 1 - k}

    def z_peer(d):
        return (z + d) % layers

    def z_dev(d):
        return {"section": s, "mp": z_peer(d) * 2 + k}

    def load(c):
        slot = c % SLOTS
        at = pl.ds(c * cc, cc)
        return (
            pltpu.make_async_copy(wg_hbm.at[0, at], wg.at[slot], w_sem.at[slot, 0]),
            pltpu.make_async_copy(wu_hbm.at[0, at], wu.at[slot], w_sem.at[slot, 1]),
        )

    def load_down():
        return (
            pltpu.make_async_copy(wd_hbm.at[0], wd, d_sem.at[0]),
            pltpu.make_async_copy(wkv_hbm, wkv, d_sem.at[1]),
        )

    for c in range(min(SLOTS, chunks)):
        for copy in load(c):
            copy.start()

    barrier = pltpu.get_barrier_semaphore()
    greet = [z_dev(d) for d in range(1, layers)] + [partner]
    greet += [{"section": (s + d) % sections, "mp": m} for d in range(1, sections)]
    for dev in greet:
        pl.semaphore_signal(barrier, inc=1, device_id=dev, device_id_type=MESH)

    floats = stream[...].astype(f32)
    normed = floats * lax.rsqrt(jnp.mean(floats * floats, axis=-1, keepdims=True) + epsilon)
    normed = (normed * ffn_gain[...]).astype(bf16)
    for c in range(chunks):
        x_all[c, k, s, z] = normed[:, c * cc : (c + 1) * cc]
    wide = normed.astype(f32)
    lane = lax.broadcasted_iota(jnp.int32, (own, LANES), 1)
    first, second = ids[:, 0:1], ids[:, 1:2]
    la, lb = jnp.zeros((own, 1), f32), jnp.zeros((own, 1), f32)
    for e in range(router_t.shape[0]):
        logit = jnp.sum(wide * router_t[e : e + 1, :].astype(f32), axis=-1, keepdims=True)
        la = la + jnp.where(first == e, logit, 0.0)
        lb = lb + jnp.where(second == e, logit, 0.0)
    share = jax.nn.sigmoid(la - lb)
    mix = jnp.where(lane == first, share, 0.0) + jnp.where(lane == second, 1.0 - share, 0.0)
    high = mix.astype(bf16)
    mix_all[k, s, z, :, 0:LANES] = high
    mix_all[k, s, z, :, LANES : 2 * LANES] = (mix - high.astype(f32)).astype(bf16)
    pl.semaphore_wait(barrier, len(greet))

    pieces = [x_all.at[0], mix_all] + [x_all.at[c] for c in range(1, chunks)]
    chunk_of = [0, None] + list(range(1, chunks))
    count = len(pieces)
    sent = []

    def remote(src, dst, ss, rs, dev):
        return pltpu.make_async_remote_copy(
            src_ref=src, dst_ref=dst, send_sem=ss, recv_sem=rs, device_id=dev, device_id_type=MESH
        )

    def go(copy):
        copy.start()
        sent.append(copy)

    def gz(i, d):
        ref = pieces[i].at[k, s, z]
        return remote(ref, ref, g_send.at[i, d - 1], g_recv.at[i, d - 1], z_dev(d))

    base = layers - 1

    def gcopy(i, j, ref, dev):
        return remote(ref, ref, g_send.at[i, base + j], g_recv.at[i, base + j], dev)

    def gx(i):
        return gcopy(i, 0, pieces[i].at[k, s], to_x)

    def gy(i):
        return gcopy(i, 1, pieces[i].at[k, s], to_y)

    def gfy(i):
        return gcopy(i, 2, pieces[i].at[k, sx, pl.ds(0, half)], to_y)

    def gfx(i):
        return gcopy(i, 3, pieces[i].at[k, sy, pl.ds(half, layers - half)], to_x)

    def gp(i, j):
        return gcopy(i, 4 + j, pieces[i].at[k, (s, sx, sy, sd)[j]], partner)

    for i in range(min(Z_AHEAD, count)):
        for d in range(1, layers):
            go(gz(i, d))

    def gather_steps(t):
        if t < count:
            for d in range(1, layers):
                gz(t, d).wait_recv()
            if t + Z_AHEAD < count:
                for d in range(1, layers):
                    go(gz(t + Z_AHEAD, d))
            go(gx(t))
            go(gy(t))
            go(gp(t, 0))
        b, f, p = (t - lag for lag in GATHER_LAG)
        if 0 <= b < count:
            gx(b).wait_recv()
            go(gfy(b))
            go(gp(b, 1))
            gy(b).wait_recv()
            go(gfx(b))
            go(gp(b, 2))
        if 0 <= f < count:
            gfy(f).wait_recv()
            gfx(f).wait_recv()
            go(gp(f, 3))
        if 0 <= p < count:
            for j in range(4):
                gp(p, j).wait_recv()

    def gate_up(c):
        slot = c % SLOTS
        for copy in load(c):
            copy.wait()

        def step(n, carry):
            at = pl.ds(pl.multiple_of(n * tile, tile), tile)
            tokens = x_all[c].reshape(rows, cc)
            g = jnp.dot(tokens, wg[slot, :, at], preferred_element_type=f32)
            u = jnp.dot(tokens, wu[slot, :, at], preferred_element_type=f32)
            if c > 0:
                g = g + gate[:, at]
                u = u + up[:, at]
            if c < chunks - 1:
                gate[:, at] = g
                up[:, at] = u
            else:
                hidden[:, at] = (g / (1.0 + jnp.exp(-g)) * u * weight[:, 0:1]).astype(bf16)
            return carry

        lax.fori_loop(0, hid // tile, step, 0)
        if c + SLOTS < chunks:
            for copy in load(c + SLOTS):
                copy.start()

    last = GATHER_LAG[2]
    for t in range(count + last):
        gather_steps(t)
        if t == last:
            for copy in load_down():
                copy.start()
        if t >= last:
            c = chunk_of[t - last]
            if c is None:
                both = mix_all[...].reshape(rows, 2 * LANES).astype(f32)
                both = both[:, 0:LANES] + both[:, LANES : 2 * LANES]
                at_lane = lax.broadcasted_iota(jnp.int32, (rows, LANES), 1)
                mine = jnp.sum(jnp.where(at_lane == s, both, 0.0), axis=-1, keepdims=True)
                weight[...] = jnp.broadcast_to(mine, (rows, LANES))
            else:
                gate_up(c)

    def rcopy(c, j, src, dst, dev):
        return remote(src, dst, r_send.at[c, j], r_recv.at[c, j], dev)

    def r_pair(c):
        return rcopy(c, 0, part.at[c, 1 - k], pair_in.at[c], partner)

    def r_xd(c):
        return rcopy(c, 1, part.at[c, k, sd, pl.ds(0, half)], xd_in.at[c], to_x)

    def r_yd(c):
        return rcopy(c, 2, part.at[c, k, sd, pl.ds(half, layers - half)], yd_in.at[c], to_y)

    def r_x(c):
        return rcopy(c, 3, part.at[c, k, sx], x_in.at[c], to_x)

    def r_y(c):
        return rcopy(c, 4, part.at[c, k, sy], y_in.at[c], to_y)

    def r_z(c, d):
        return rcopy(c, 5 + d, part.at[c, k, s, z_peer(d)], z_in.at[c, d - 1], z_dev(d))

    def a_z(c, d):
        ref = attn.at[c, k, z]
        return rcopy(c, 5 + base + d, ref, ref, z_dev(d))

    def a_pair(c):
        ref = attn.at[c, k]
        return rcopy(c, 5, ref, ref, partner)

    def down(c):
        for n in range(cc // tile):
            lo = c * cc + n * tile
            r = jnp.dot(hidden[...], wd[:, lo : lo + tile], preferred_element_type=f32)
            part[c, :, :, :, :, n * tile : (n + 1) * tile] = r.astype(bf16).reshape(
                2, sections, layers, own, tile
            )

    def plus(a, b):
        return (a.astype(f32) + b.astype(f32)).astype(bf16)

    group = 2 * layers * own
    state = {"kv": jnp.zeros((group, wkv.shape[1]), f32), "ss": jnp.zeros((group, 1), f32)}

    for copy in load_down():
        copy.wait()
    for t in range(chunks + RETURN_LAG[5]):
        l1, l2, l3, l4, l5, l6 = (t - lag for lag in RETURN_LAG)
        if 0 <= l5 < chunks:
            for d in range(1, layers):
                a_z(l5, d).wait_recv()
            go(a_pair(l5))
        if 0 <= l4 < chunks:
            c = l4
            cols = slice(c * cc, (c + 1) * cc)
            total = part[c, k, s, z].astype(f32)
            for d in range(1, layers):
                r_z(c, d).wait_recv()
                total = total + z_in[c, d - 1].astype(f32)
            updated = (stream[:, cols].astype(f32) + total).astype(bf16)
            attn[c, k, z] = updated
            for d in range(1, layers):
                go(a_z(c, d))
            out[:, cols] = updated
        if 0 <= l3 < chunks:
            c = l3
            r_x(c).wait_recv()
            r_y(c).wait_recv()
            add = part[c, k, s].astype(f32) + x_in[c].astype(f32) + y_in[c].astype(f32)
            part[c, k, s] = add.astype(bf16)
            for d in range(1, layers):
                go(r_z(c, d))
        if 0 <= l2 < chunks:
            c = l2
            r_xd(c).wait_recv()
            part[c, k, sy, 0:half] = plus(part[c, k, sy, 0:half], xd_in[c])
            go(r_y(c))
            r_yd(c).wait_recv()
            part[c, k, sx, half:layers] = plus(part[c, k, sx, half:layers], yd_in[c])
            go(r_x(c))
        if 0 <= l1 < chunks:
            c = l1
            r_pair(c).wait_recv()
            part[c, k] = plus(part[c, k], pair_in[c])
            go(r_xd(c))
            go(r_yd(c))
        if t < chunks:
            down(t)
            go(r_pair(t))
        if 0 <= l6 < chunks:
            c = l6
            cols = slice(c * cc, (c + 1) * cc)
            a_pair(c).wait_recv()
            values = attn[c].reshape(group, cc).astype(f32)
            state["ss"] = state["ss"] + jnp.sum(values * values, axis=-1, keepdims=True)
            scaled = (values * attn_gain[:, cols]).astype(bf16)
            state["kv"] = state["kv"] + jnp.dot(scaled, wkv[cols, :], preferred_element_type=f32)
    keys = state["kv"] * lax.rsqrt(state["ss"] / width + epsilon)
    keys = keys.astype(bf16).reshape(2, layers, own, wkv.shape[1])
    for core in range(2):
        for layer in range(layers):
            at = (layer * 2 + core) * own
            kv_mine[at : at + own, :] = keys[core, layer]
    onward = remote(
        kv_mine, kv_in, k_send.at[0], k_recv.at[0], {"section": (s + 1) % sections, "mp": m}
    )
    go(onward)
    onward.wait_recv()
    kv_out[...] = kv_in[...]
    for copy in sent:
        copy.wait_send()


def fused_body(sections, mp, chunks, stream, ffn_gain, router_weight, expert_ids, w_gate, w_up, w_down, attn_gain, w_kv):
    own, width = stream.shape
    layers = mp // 2
    cc = width // chunks
    hid = w_gate.shape[2]
    rows = sections * mp * own
    kvc = w_kv.shape[1]
    vmem = pl.BlockSpec(memory_space=pltpu.VMEM)
    hbm = pl.BlockSpec(memory_space=pl.ANY)
    dma = pltpu.SemaphoreType.DMA
    gathers, returns = layers - 1 + 8, 5 + 2 * layers - 1
    flops = 6 * rows * width * hid
    return pl.pallas_call(
        functools.partial(fused_kernel, sections, layers, chunks),
        out_shape=(
            jax.ShapeDtypeStruct((own, width), bf16),
            jax.ShapeDtypeStruct((mp * own, kvc), bf16),
        ),
        in_specs=[vmem] * 5 + [hbm] * 4,
        out_specs=(vmem, vmem),
        scratch_shapes=[
            pltpu.VMEM((chunks, 2, sections, layers, own, cc), bf16),
            pltpu.VMEM((2, sections, layers, own, 2 * LANES), bf16),
            pltpu.VMEM((SLOTS, cc, hid), bf16),
            pltpu.VMEM((SLOTS, cc, hid), bf16),
            pltpu.VMEM((hid, width), bf16),
            pltpu.VMEM((width, kvc), bf16),
            pltpu.VMEM((rows, hid), f32),
            pltpu.VMEM((rows, hid), f32),
            pltpu.VMEM((rows, hid), bf16),
            pltpu.VMEM((chunks, 2, sections, layers, own, cc), bf16),
            pltpu.VMEM((chunks, sections, layers, own, cc), bf16),
            pltpu.VMEM((chunks, layers // 2, own, cc), bf16),
            pltpu.VMEM((chunks, layers - layers // 2, own, cc), bf16),
            pltpu.VMEM((chunks, layers, own, cc), bf16),
            pltpu.VMEM((chunks, layers, own, cc), bf16),
            pltpu.VMEM((chunks, layers - 1, own, cc), bf16),
            pltpu.VMEM((chunks, 2, layers, own, cc), bf16),
            pltpu.VMEM((mp * own, kvc), bf16),
            pltpu.VMEM((mp * own, kvc), bf16),
            pltpu.VMEM((rows, LANES), f32),
            dma((chunks + 1, gathers)),
            dma((chunks + 1, gathers)),
            dma((chunks, returns)),
            dma((chunks, returns)),
            dma((SLOTS, 2)),
            dma((2,)),
            dma((1,)),
            dma((1,)),
        ],
        compiler_params=pltpu.CompilerParams(
            collective_id=0, has_side_effects=True, vmem_limit_bytes=VMEM_BYTES
        ),
        cost_estimate=pl.CostEstimate(
            flops=flops, bytes_accessed=6 * width * hid, transcendentals=rows * hid
        ),
        name="expert_feed_forward",
    )(
        stream, ffn_gain[None, :], router_weight.T, expert_ids, attn_gain[None, :],
        w_gate, w_up, w_down, w_kv,
    )


def body(sections, mp, *args):
    stream, router_weight, w_gate = args[0], args[2], args[4]
    own, width = stream.shape
    rows, hid = sections * mp * own, w_gate.shape[2]
    chunks = width // 512
    held = rows * width * 7 + rows * hid * 10 + width * hid * 2 + SLOTS * 2048 * hid
    fits = held < VMEM_BYTES - (6 << 20)
    shaped = sections == 4 and mp % 4 == 0 and own % 16 == 0 and width % 512 == 0
    shaped = shaped and hid % LANES == 0 and router_weight.shape[1] == sections
    if fits and shaped:
        return fused_body(sections, mp, chunks, *args)
    return plain_body(*args)


def solution(mesh):
    in_specs = (
        P(("section", "mp"), None),
        P(),
        P(),
        P(("section", "mp"), None),
        P("section", None, "mp"),
        P("section", None, "mp"),
        P("section", "mp", None),
        P(),
        P(None, "mp"),
    )
    out_specs = (P(("section", "mp"), None), P("section", "mp"))
    return jax.shard_map(
        functools.partial(body, mesh.shape["section"], mesh.shape["mp"]), mesh=mesh, in_specs=in_specs, out_specs=out_specs, check_vma=False)
```
